32 devices in a mesh: row: 8 (over z, x), col: 4 (over y, core).
Axes of the slice: x: 2, y: 2, z: 4, core: 2. Of those that a mesh axis runs over, the one named last changes fastest.
Arguments:
- forward_map: float32 [2048, 16384], P('row', 'col'), may hold values from -0.125 to 0.125
- sensor_weights: float32 [2048], P('row'), may hold values from 0.25 to 4
- sensor_mask: int32 [2048], P('row'), may hold values 0 or 1
Outputs:
- gram_matrix: float32 [16384, 16384], P('row', 'col')
The draws below stay inside these ranges and needn't reach their ends.
All inputs are finite; a program needn't handle non-finite values. No bound on the sum of `sensor_mask` on one device may be relied on, other than what follows from the above.
Results may differ from the reference program's by a relative error of at most 0.000061.
Values sent between devices are 32-bit elements; how exact they have to be, the bound alone decides.
No kernel may reach another device: no remote copies, remote signals or barrier semaphores. Data moves between devices by JAX's collectives and lax.ppermute only.
A program may use at most 128 MiB of HBM per device.

```python
import math
import jax
import jax.numpy as jnp
from jax import lax

PARAMS = 16384
OBS = 2048


def with_ends(array, stream_key, least, largest):
    longest = array.shape.index(max(array.shape))
    spots = []
    for shift in (0, 1):
        where = [jax.random.randint(jax.random.fold_in(stream_key, axis), (), 0, length) for axis, length in enumerate(array.shape)]
        where[longest] = (where[longest] + shift) % array.shape[longest]
        spots.append(tuple(where))
    return array.at[spots[0]].set(least).at[spots[1]].set(largest)


def level_of(own_key, extent, shards, least, largest):
    level, own = 1.0, jax.random.fold_in(own_key, 6)
    for dim, shards_of in shards:
        steps = jnp.exp(jax.random.uniform(jax.random.fold_in(own, dim), (shards_of,), jnp.float32, least / len(shards), largest / len(shards)))
        level = level * jnp.repeat(steps, extent[dim] // shards_of).reshape([-1 if axis == dim else 1 for axis in range(len(extent))])
    return level


def centred(own_key, shape, width, most, pieces=(), held_as=jnp.bfloat16):
    gain = level_of(own_key, shape, pieces, -0.22, 0.18) if pieces else 1.0
    result = jax.random.normal(own_key, shape, jnp.float32) * width * gain
    return jnp.minimum(jnp.maximum(result, -most), most).astype(held_as)


def setup_inputs(seed: int = 0) -> dict:
    key_of = jax.random.split(jax.random.key(seed), 4)
    return {
        "forward_map": centred(key_of[0], (OBS, PARAMS), OBS ** -0.5, 0.125, ((0, 8), (1, 4)), jnp.float32),
        "sensor_weights": jnp.clip(jnp.exp(math.log(4.0) - 2.7725887 * jax.random.uniform(key_of[1], (OBS,), jnp.float32) ** level_of(key_of[1], (OBS,), ((0, 8),), -0.2, 0.2)), 0.25, 4.0),
        "sensor_mask": with_ends((jax.random.randint(key_of[2], (OBS,), 0, 2) < 1).astype(jnp.int32), jax.random.fold_in(key_of[2], 1), 0, 1),
    }


def reference(forward_map, sensor_weights, sensor_mask):
    sensor_scale = sensor_weights * sensor_mask.astype(jnp.float32)
    weighted = forward_map * sensor_scale[:, None]
    return lax.dot_general(forward_map, weighted, (((0,), (0,)), ((), ())), precision=lax.Precision.HIGHEST, preferred_element_type=jnp.float32)
```

```python
import functools

import jax
import jax.numpy as jnp
from jax import lax
from jax.experimental import pallas as pl
from jax.experimental.pallas import tpu as pltpu
from jax.sharding import PartitionSpec as P


INTERPRET = False


def add_kernel(a_ref, b_ref, acc_ref, out_ref, *, chunk):
    def body(step, carry):
        columns = pl.ds(pl.multiple_of(step * chunk, chunk), chunk)
        product = jnp.dot(a_ref[...], b_ref[:, columns], preferred_element_type=jnp.float32)
        out_ref[:, columns] = product if acc_ref is None else acc_ref[:, columns] + product
        return carry

    lax.fori_loop(0, out_ref.shape[1] // chunk, body, 0)


def first_kernel(a_ref, b_ref, out_ref, *, chunk):
    add_kernel(a_ref, b_ref, None, out_ref, chunk=chunk)


def accumulate(acc, a, b):
    depth, width = b.shape
    height = a.shape[0]
    tile = min(height, 256)
    chunk = min(width, 512)
    block = pl.BlockSpec((tile, width), lambda i: (i, 0))
    specs = [
        pl.BlockSpec((tile, depth), lambda i: (i, 0)),
        pl.BlockSpec((depth, width), lambda i: (0, 0)),
    ]
    given = acc is not None
    return pl.pallas_call(
        functools.partial(add_kernel if given else first_kernel, chunk=chunk),
        grid=(height // tile,),
        in_specs=specs + [block] * given,
        out_specs=block,
        out_shape=jax.ShapeDtypeStruct((height, width), jnp.float32),
        input_output_aliases={2: 0} if given else {},
        compiler_params=pltpu.CompilerParams(vmem_limit_bytes=50 * 2**20),
        cost_estimate=pl.CostEstimate(
            flops=2 * height * width * depth,
            bytes_accessed=4 * height * width * (1 + given) + 2 * depth * (height + width),
            transcendentals=0,
        ),
        interpret=INTERPRET,
    )(a, b, *([acc] if given else []))


def halves(x):
    high = lax.reduce_precision(x, 8, 7)
    return high.astype(jnp.bfloat16), (x - high).astype(jnp.bfloat16)


def contribute(acc, left, right):
    left_high, left_low = halves(left)
    right_high, right_low = halves(right)
    a = jnp.concatenate([left_high, left_high, left_low], axis=0).T
    b = jnp.concatenate([right_high, right_low, right_high], axis=0)
    return accumulate(acc, a, b)


def per_layer(forward_map, sensor_weights, sensor_mask):
    rows = lax.axis_size("row")
    cols = lax.axis_size("col")
    row = lax.axis_index("row")
    col = lax.axis_index("col")
    height, width = forward_map.shape
    span = width * cols // rows
    per_col = width // span
    assert per_col * span == width and cols & (cols - 1) == 0

    order = list(range(0, rows, 2)) + list(range(1, rows, 2))[::-1]
    ahead = [(order[i], order[(i + 1) % rows]) for i in range(rows)]
    back = [(there, here) for here, there in ahead]

    source = row // per_col
    offset = (row % per_col) * span

    def spread(piece):
        held = lax.dynamic_slice(piece, (0, offset), (piece.shape[0], span))
        known, bit = 0, cols // 2
        while bit:
            pairs = []
            for r in range(rows):
                origin = r // per_col
                for c in range(cols):
                    if (c ^ origin) & ~known == 0:
                        pairs.append((r * cols + c, r * cols + (c ^ bit)))
            received = lax.ppermute(held, ("row", "col"), pairs)
            has = ((col ^ source) & ~known) == 0
            held = jnp.where(has, held, received)
            known |= bit
            bit //= 2
        return held

    scale = jnp.sqrt(sensor_weights * sensor_mask.astype(jnp.float32))
    index = lax.broadcasted_iota(jnp.int32, (height, height), 0)
    other = lax.broadcasted_iota(jnp.int32, (height, height), 1)
    before = jnp.sum(jnp.where(index < other, sensor_mask[:, None], 0), axis=0)
    count = jnp.sum(sensor_mask)

    def selected(start, amount):
        wanted = start + lax.broadcasted_iota(jnp.int32, (amount, height), 0)
        pick = (before[None, :] == wanted) & (sensor_mask[None, :] != 0)
        return lax.dot_general(
            jnp.where(pick, scale[None, :], 0.0),
            forward_map,
            (((1,), (0,)), ((), ())),
            precision=lax.Precision.HIGHEST,
            preferred_element_type=jnp.float32,
        )

    room = min(height, -(-height * 9 // 256) * 16)
    own = selected(0, room)
    most = lax.pmax(count, "row")
    up, down = own[: room // 2], own[room // 2 :]
    acc = None
    pending = [(spread(own), own)]
    for step in range(1, rows):
        up = lax.ppermute(up, "row", ahead)
        down = lax.ppermute(down, "row", back)
        right = jnp.concatenate([up, down], axis=0)
        pending.append((spread(right), right))
        if len(pending) == 2 or step == rows - 1:
            left = jnp.concatenate([piece for piece, _ in pending], axis=0)
            right = jnp.concatenate([piece for _, piece in pending], axis=0)
            acc = contribute(acc, left, right)
            pending = []

    extra = 16
    if room < height:

        def more(step, total):
            block = selected(room + step * extra, extra)
            gathered = lax.all_gather(block, "row", axis=0, tiled=True)
            return contribute(total, spread(gathered), gathered)

        steps = jnp.maximum(most - room + extra - 1, 0) // extra
        acc = lax.fori_loop(0, steps, more, acc)
    return acc


def solution(mesh):
    placed = (P("row", "col"), P("row"), P("row"))
    return jax.shard_map(
        per_layer, mesh=mesh, in_specs=placed, out_specs=P("row", "col"), check_vma=False
    )
```
